32 devices in a mesh: expert: 4 (over y, core), shard: 8 (over z, x).
Axes of the slice: x: 2, y: 2, z: 4, core: 2. Of those that a mesh axis runs over, the one named last changes fastest.
Arguments:
- master_gate: float32 [128, 2048, 768], P('expert', 'shard'), may hold values from -0.125 to 0.125
- second_gate: bfloat16 [128, 2048, 768], P('expert', 'shard'), may hold values from -0.0625 to 0.0625
- master_up: float32 [128, 2048, 768], P('expert', 'shard'), may hold values from -0.125 to 0.125
- second_up: bfloat16 [128, 2048, 768], P('expert', 'shard'), may hold values from -0.0625 to 0.0625
- router_weight: float32 [2048, 128], P('shard', 'expert'), may hold values from -0.125 to 0.125
- router_gain: float32 [2048], P('shard'), may hold values from 0.25 to 1.75
Outputs:
- final_gate: bfloat16 [128, 768, 2048], P('expert', 'shard')
- final_up: bfloat16 [128, 768, 2048], P('expert', 'shard')
- serve_router: bfloat16 [2048, 128], replicated
The draws below stay inside these ranges and needn't reach their ends.
All inputs are finite; a program needn't handle non-finite values.
Results may differ from the reference program's by a relative error of at most 0.001.
Values may be sent and summed in bfloat16 or wider, within the bound.
A program may use at most 192 MiB of HBM per device.

```python
import jax
import jax.numpy as jnp

EXPERTS = 128
D_MODEL = 2048
D_EXPERT = 768


def levels(rng, dims, split, low, high):
    def one(position, shards_of):
        draws = jax.random.uniform(jax.random.fold_in(jax.random.fold_in(rng, 6), position), (shards_of,), jnp.float32, low / len(split), high / len(split))
        return jnp.repeat(jnp.exp(draws), dims[position] // shards_of).reshape((-1,) + (1,) * (len(dims) - position - 1))

    gain = one(*split[0])
    for cut in split[1:]:
        gain = gain * one(*cut)
    return gain


def scatter_about(stream_key, shape, spread, most, cuts=(), held_as=jnp.bfloat16):
    array = jax.random.normal(stream_key, shape, jnp.float32) * spread
    if len(cuts) > 0:
        array = levels(stream_key, shape, cuts, -0.22, 0.18) * array
    return jnp.clip(array, min=-most, max=most).astype(held_as)


def setup_inputs(seed: int = 0) -> dict:
    arg_keys = jax.random.split(jax.random.key(seed), 7)
    master_gate = scatter_about(arg_keys[0], (EXPERTS, D_MODEL, D_EXPERT), D_MODEL ** -0.5, 0.125, ((0, 4), (1, 8)), jnp.float32)
    second_gate = scatter_about(arg_keys[1], (EXPERTS, D_MODEL, D_EXPERT), (D_MODEL * 4) ** -0.5, 0.0625, ((0, 4), (1, 8)))
    master_up = scatter_about(arg_keys[2], (EXPERTS, D_MODEL, D_EXPERT), D_MODEL ** -0.5, 0.125, ((0, 4), (1, 8)), jnp.float32)
    second_up = scatter_about(arg_keys[3], (EXPERTS, D_MODEL, D_EXPERT), (D_MODEL * 4) ** -0.5, 0.0625, ((0, 4), (1, 8)))
    router_weight = scatter_about(arg_keys[4], (D_MODEL, EXPERTS), D_MODEL ** -0.5, 0.125, ((0, 8), (1, 4)), jnp.float32)
    router_gain = jnp.clip(1.0 + 0.15 * jax.random.normal(arg_keys[5], (D_MODEL,), jnp.float32), 0.25, 1.75)
    return dict(master_gate=master_gate, second_gate=second_gate, master_up=master_up, second_up=second_up, router_weight=router_weight, router_gain=router_gain)


def reference(master_gate, second_gate, master_up, second_up, router_weight, router_gain):
    merged_gate = master_gate + second_gate.astype(jnp.float32)
    merged_up = master_up + second_up.astype(jnp.float32)
    final_gate = merged_gate.astype(jnp.bfloat16)
    final_gate = jnp.transpose(final_gate, (0, 2, 1))
    final_up = merged_up.astype(jnp.bfloat16)
    final_up = jnp.transpose(final_up, (0, 2, 1))
    serve_router = (router_weight * router_gain[:, None]).astype(jnp.bfloat16)
    return final_gate, final_up, serve_router
```

```python
import functools

import jax
import jax.numpy as jnp
from jax import lax
from jax.experimental import pallas as pl
from jax.experimental.pallas import tpu as pltpu
from jax.sharding import PartitionSpec as P

SLOTS = 12
LOADS = 2
SECOND = 4
HELD = 13
MESH_IDS = pl.DeviceIdType.MESH


def plain(master_gate, second_gate, master_up, second_up, router_weight, router_gain):
    merged_gate = master_gate + second_gate.astype(jnp.float32)
    merged_up = master_up + second_up.astype(jnp.float32)
    narrow_gate, narrow_up = (merged_gate.astype(jnp.bfloat16), merged_up.astype(jnp.bfloat16))
    final_gate, final_up = (
        lax.all_to_all(narrow_gate, "shard", split_axis=2, concat_axis=1, tiled=True),
        lax.all_to_all(narrow_up, "shard", split_axis=2, concat_axis=1, tiled=True),
    )
    final_gate = jnp.transpose(final_gate, (0, 2, 1))
    final_up = jnp.transpose(final_up, (0, 2, 1))
    part_router = (router_weight * router_gain[:, None]).astype(jnp.bfloat16)
    row_router = lax.all_gather(part_router, "shard", axis=0, tiled=True)
    serve_router = lax.all_gather(row_router, "expert", axis=1, tiled=True)
    return (final_gate, final_up, serve_router)


def peers(me, n):
    half, quarter = n // 2, n // 4
    mine, place, x = me // half, me % half, me % quarter
    is_end = (place // quarter) == mine
    far_end = [(1 - mine) * (n - quarter) + (x + i) % quarter for i in range(quarter)]
    far_mid = [half - mine * quarter + (x + i) % quarter for i in range(quarter)]
    near = [mine * half + (place + i) % half for i in range(1, half)]
    return is_end, far_end, far_mid, near


def regroup_kernel(n, groups, mg, sg, mu, su, rw, gain, og, ou, orr, stash,
                   in_m, in_s, stage, rw_v, gain_v, r_part, r_all,
                   load_m, load_s, load_r, send, own, recv, r_send, r_recv, f_send, f_recv):
    experts, rows, inner = mg.shape
    part = inner // n
    r_cols = rw.shape[0]
    group, me = lax.axis_index("expert"), lax.axis_index("shard")
    is_end, far_end, far_mid, near = peers(me, n)
    mirror_x = jnp.where(is_end, far_end[0], far_mid[0])
    to = far_end + far_mid + near
    quarter = n // 4
    total = 2 * experts
    other = [(group + i) % groups for i in range(1, groups)]
    masters, seconds, outs = (mg, mu), (sg, su), (og, ou)
    home = pl.ds(pl.multiple_of(me * rows, rows), rows)

    def loads(a, e):
        slot = e % LOADS
        return (
            pltpu.make_async_copy(masters[a].at[e], in_m.at[a, slot], load_m.at[a, slot]),
            pltpu.make_async_copy(seconds[a].at[e], in_s.at[a, slot], load_s.at[a, slot]),
        )

    def start_loads(a, e):
        for copy in loads(a, e):
            copy.start()

    def router_loads():
        return (
            pltpu.make_async_copy(rw, rw_v, load_r.at[0]),
            pltpu.make_async_copy(gain, gain_v, load_r.at[1]),
        )

    def block(a, e, device):
        src = pl.ds(pl.multiple_of(device * part, part), part)
        return stage.at[a, e % SLOTS, src, :], outs[a].at[e, :, home]

    def send_to(a, e, devices):
        for device in devices:
            src, dst = block(a, e, device)
            pltpu.make_async_remote_copy(
                src_ref=src, dst_ref=dst, send_sem=send.at[a, e % SLOTS], recv_sem=recv.at[a, e],
                device_id=(group, device), device_id_type=MESH_IDS,
            ).start()

    def seconds_of(a, e):
        return is_end & (2 * e + a >= total - SECOND)

    def start_sends(a, e):
        m = 2 * e + a

        @pl.when(~seconds_of(a, e))
        def _():
            send_to(a, e, far_end)

        for i, device in enumerate(far_mid):
            @pl.when(is_end | (m * quarter + i < total * quarter - HELD))
            def _():
                send_to(a, e, [device])

        send_to(a, e, near)
        src, dst = block(a, e, me)
        pltpu.make_async_copy(src, dst, own.at[a, e % SLOTS]).start()

    def wait_sends(a, e, blocks=n - 1):
        many = stage.at[a, e % SLOTS, pl.ds(0, blocks * part), :]
        pltpu.make_async_copy(many, many, send.at[a, e % SLOTS]).wait()
        src, dst = block(a, e, me)
        pltpu.make_async_copy(src, dst, own.at[a, e % SLOTS]).wait()

    def merge(a, e):
        for copy in loads(a, e):
            copy.wait()

        @pl.when(e >= SLOTS)
        def _():
            wait_sends(a, e - SLOTS)

        slot, into = e % LOADS, e % SLOTS
        for c in range(inner // 128):
            cols = slice(c * 128, (c + 1) * 128)
            merged = in_m[a, slot, :, cols] + in_s[a, slot, :, cols].astype(jnp.float32)
            stage[a, into, cols, :] = merged.T.astype(jnp.bfloat16)

        @pl.when(2 * e + a >= total - SECOND)
        def _():
            theirs = pl.ds(pl.multiple_of((1 - me // (n // 2)) * (n - quarter) * part, quarter * part), quarter * part)
            stash[2 * e + a - (total - SECOND)] = stage[a, into, theirs, :]

        @pl.when(e + LOADS < experts)
        def _():
            start_loads(a, e + LOADS)

    for a in range(2):
        start_loads(a, 0)
    for copy in router_loads():
        copy.start()
    for e in range(1, LOADS):
        for a in range(2):
            start_loads(a, e)

    barrier = pltpu.get_barrier_semaphore()
    for device in to:
        pl.semaphore_signal(barrier, inc=1, device_id=(group, device), device_id_type=MESH_IDS)
    for g in other:
        pl.semaphore_signal(barrier, inc=1, device_id=(g, me), device_id_type=MESH_IDS)

    merge(0, 0)
    for copy in router_loads():
        copy.wait()
    mine = (rw_v[...] * gain_v[...]).astype(jnp.bfloat16)
    r_rows = pl.ds(pl.multiple_of(group * r_cols, r_cols), r_cols)
    r_part[...] = mine
    r_all[r_rows, home] = mine
    pl.semaphore_wait(barrier, len(to) + len(other))
    start_sends(0, 0)
    merge(1, 0)

    def hand(src, dst, i, device):
        pltpu.make_async_remote_copy(
            src_ref=src, dst_ref=dst, send_sem=r_send.at[i], recv_sem=r_recv.at[i],
            device_id=(group, device), device_id_type=MESH_IDS,
        ).start()

    def wait_hands(sems, i, count):
        many = r_all.at[pl.ds(0, r_cols), pl.ds(0, count * rows)]
        pltpu.make_async_copy(many, many, sems.at[i]).wait()

    hand(r_part, r_all.at[r_rows, home], 0, mirror_x)
    for device in near:
        hand(r_part, r_all.at[r_rows, home], 1, device)

    def step(e, carry):
        merge(0, e)
        start_sends(1, e - 1)
        merge(1, e)
        start_sends(0, e)
        return carry

    lax.fori_loop(1, experts, step, 0)

    start_sends(1, experts - 1)

    @pl.when(~is_end)
    def _():
        for i in range(total * quarter - HELD, total * quarter):
            m = i // quarter
            send_to(m % 2, m // 2, [far_mid[i % quarter]])

    wait_hands(r_recv, 0, 1)
    mirror = r_all.at[r_rows, pl.ds(pl.multiple_of(mirror_x * rows, rows), rows)]
    for device in near:
        hand(mirror, mirror, 2, device)
    wait_hands(r_send, 0, 1)
    for i in (1, 2):
        wait_hands(r_recv, i, len(near))
        wait_hands(r_send, i, len(near))
    for g in other:
        pltpu.make_async_remote_copy(
            src_ref=r_all.at[r_rows, :], dst_ref=r_all.at[r_rows, :], send_sem=f_send, recv_sem=f_recv,
            device_id=(g, me), device_id_type=MESH_IDS,
        ).start()
    many = r_all.at[pl.ds(0, (groups - 1) * r_cols), :]
    pltpu.make_async_copy(many, many, f_recv).wait()
    pltpu.make_async_copy(many, many, f_send).wait()
    for c in range(orr.shape[0] // 128):
        span = slice(c * 128, (c + 1) * 128)
        orr[span, :] = r_all[:, span].astype(jnp.float32).T.astype(jnp.bfloat16)

    def drain(e, carry):
        for a in range(2):
            @pl.when(seconds_of(a, e))
            def _():
                wait_sends(a, e, n - 1 - quarter)

            @pl.when(~seconds_of(a, e))
            def _():
                wait_sends(a, e)
        return carry

    lax.fori_loop(max(experts - SLOTS, 0), experts, drain, 0)

    def wait_recv(a, e, blocks):
        many = outs[a].at[e, :, pl.ds(0, blocks * rows)]
        pltpu.make_async_copy(many, many, recv.at[a, e]).wait()

    def arrive(e, carry):
        for a in range(2):
            @pl.when(seconds_of(a, e))
            def _():
                wait_recv(a, e, n - 1 - quarter)

            @pl.when(~seconds_of(a, e))
            def _():
                wait_recv(a, e, n - 1)
        return carry

    lax.fori_loop(0, experts, arrive, 0)


def second_kernel(n, stash, after, land, send, recv):
    group, me = lax.axis_index("expert"), lax.axis_index("shard")
    is_end, far_end, _, _ = peers(me, n)
    quarter = n // 4
    part, rows = stash.shape[1] // quarter, stash.shape[2]
    x = me % quarter
    barrier = pltpu.get_barrier_semaphore()

    @pl.when(is_end)
    def _():
        for device in far_end:
            pl.semaphore_signal(barrier, inc=1, device_id=(group, device), device_id_type=MESH_IDS)
        pl.semaphore_wait(barrier, quarter)
        for m in range(SECOND):
            for device in far_end:
                pltpu.make_async_remote_copy(
                    src_ref=stash.at[m, pl.ds(pl.multiple_of(device % quarter * part, part), part), :],
                    dst_ref=land.at[m, :, pl.ds(pl.multiple_of(x * rows, rows), rows)],
                    send_sem=send, recv_sem=recv, device_id=(group, device), device_id_type=MESH_IDS,
                ).start()
        pltpu.make_async_copy(land, land, recv).wait()
        pltpu.make_async_copy(stash, stash, send).wait()


def second(n, stash, after):
    _, span, rows = stash.shape
    quarter = n // 4
    anywhere = pl.BlockSpec(memory_space=pl.ANY)
    return pl.pallas_call(
        functools.partial(second_kernel, n),
        out_shape=pltpu.VMEM((SECOND, span // quarter, quarter * rows), stash.dtype),
        in_specs=[anywhere, anywhere],
        out_specs=anywhere,
        scratch_shapes=[pltpu.SemaphoreType.DMA, pltpu.SemaphoreType.DMA],
        compiler_params=pltpu.CompilerParams(
            collective_id=1, has_side_effects=True, vmem_limit_bytes=1024 * 1024,
        ),
        name="second",
    )(stash, after)


def fill_kernel(n, gate, up, land, og, ou, done):
    me = lax.axis_index("shard")
    is_end, _, _, _ = peers(me, n)
    half, quarter = n // 2, n // 4
    experts, width = gate.shape[0], land.shape[2]
    spot = pl.ds(pl.multiple_of((1 - me // half) * (n - quarter) * (width // quarter), width), width)

    @pl.when(is_end)
    def _():
        copies = []
        for i in range(SECOND):
            m = 2 * experts - SECOND + i
            copies.append(pltpu.make_async_copy(land.at[i], (og, ou)[m % 2].at[m // 2, :, spot], done.at[i]))
        for copy in copies:
            copy.start()
        for copy in copies:
            copy.wait()


def fill(n, gate, up, land):
    anywhere = pl.BlockSpec(memory_space=pl.ANY)
    return pl.pallas_call(
        functools.partial(fill_kernel, n),
        out_shape=tuple(pltpu.HBM(x.shape, x.dtype) for x in (gate, up)),
        in_specs=[anywhere] * 3,
        out_specs=(anywhere,) * 2,
        scratch_shapes=[pltpu.SemaphoreType.DMA((SECOND,))],
        input_output_aliases={0: 0, 1: 1},
        compiler_params=pltpu.CompilerParams(vmem_limit_bytes=1024 * 1024),
        name="fill",
    )(gate, up, land)


PIECES = 4


def put_kernel(gate, up, router, og, ou, orr, after, done, done_router):
    size = gate.shape[0] // PIECES
    copies = [
        pltpu.make_async_copy(src.at[pl.ds(i * size, size)], dst.at[pl.ds(i * size, size)], done.at[a, i])
        for i in range(PIECES)
        for a, (src, dst) in enumerate(((gate, og), (up, ou)))
    ]
    copies.append(pltpu.make_async_copy(router, orr, done_router))
    for copy in copies:
        copy.start()
    for copy in copies:
        copy.wait()


def put(*held):
    anywhere = pl.BlockSpec(memory_space=pl.ANY)
    return pl.pallas_call(
        put_kernel,
        out_shape=tuple(pltpu.HBM(x.shape, x.dtype) for x in held) + (pltpu.VMEM((8, 128), jnp.float32),),
        in_specs=[anywhere] * len(held),
        out_specs=(anywhere,) * (len(held) + 1),
        scratch_shapes=[pltpu.SemaphoreType.DMA((2, PIECES)), pltpu.SemaphoreType.DMA],
        compiler_params=pltpu.CompilerParams(vmem_limit_bytes=1024 * 1024),
        name="put",
    )(*held)


def fused(n, groups, master_gate, second_gate, master_up, second_up, router_weight, router_gain):
    experts, rows, inner = master_gate.shape
    r_cols = router_weight.shape[1]
    final = (experts, inner // n, rows * n)
    anywhere = pl.BlockSpec(memory_space=pl.ANY)
    dma = pltpu.SemaphoreType.DMA
    *held, stash = pl.pallas_call(
        functools.partial(regroup_kernel, n, groups),
        out_shape=(
            pltpu.VMEM(final, jnp.bfloat16),
            pltpu.VMEM(final, jnp.bfloat16),
            jax.ShapeDtypeStruct((rows * n, r_cols * groups), jnp.bfloat16),
            pltpu.VMEM((SECOND, inner // 4, rows), jnp.bfloat16),
        ),
        in_specs=[anywhere] * 6,
        out_specs=(anywhere, anywhere, pl.BlockSpec(memory_space=pltpu.VMEM), pl.BlockSpec(memory_space=pltpu.VMEM)),
        scratch_shapes=[
            pltpu.VMEM((2, LOADS, rows, inner), jnp.float32),
            pltpu.VMEM((2, LOADS, rows, inner), jnp.bfloat16),
            pltpu.VMEM((2, SLOTS, inner, rows), jnp.bfloat16),
            pltpu.VMEM((r_cols, rows), jnp.float32),
            pltpu.VMEM((1, rows), jnp.float32),
            pltpu.VMEM((r_cols, rows), jnp.bfloat16),
            pltpu.VMEM((r_cols * groups, rows * n), jnp.bfloat16),
            dma((2, LOADS)), dma((2, LOADS)), dma((2,)),
            dma((2, SLOTS)), dma((2, SLOTS)), dma((2, experts)),
            dma((3,)), dma((3,)), dma, dma,
        ],
        compiler_params=pltpu.CompilerParams(
            collective_id=0, has_side_effects=True, vmem_limit_bytes=24 * 1024 * 1024,
        ),
        name="regroup",
    )(
        master_gate, second_gate, master_up, second_up,
        pltpu.with_memory_space_constraint(router_weight.T, pltpu.HBM),
        pltpu.with_memory_space_constraint(router_gain[None, :], pltpu.HBM),
    )
    gate, up, router, after = put(*held)
    return *fill(n, gate, up, second(n, stash, after)), router


def solution(mesh):
    n, groups = mesh.shape["shard"], mesh.shape["expert"]

    def shards(*args):
        experts, rows, inner = args[0].shape
        r_cols = args[4].shape[1]
        fits = (
            n % 4 == 0 and groups > 1 and rows % 128 == 0 and inner % 128 == 0
            and (inner // n) % 16 == 0 and r_cols % 16 == 0 and experts % PIECES == 0 and experts >= max(SLOTS, LOADS) and 2 * SLOTS * (n // 4) > HELD + n // 2
        )
        return fused(n, groups, *args) if fits else plain(*args)

    in_specs = (
        P("expert", "shard", None),
        P("expert", "shard", None),
        P("expert", "shard", None),
        P("expert", "shard", None),
        P("shard", "expert"),
        P("shard"),
    )
    out_specs = (P("expert", "shard", None), P("expert", "shard", None), P())
    return jax.shard_map(shards, mesh=mesh, in_specs=in_specs, out_specs=out_specs, check_vma=False)
```

```python
import functools

import jax
import jax.numpy as jnp
from jax import lax
from jax.experimental import pallas as pl
from jax.experimental.pallas import tpu as pltpu
from jax.sharding import PartitionSpec as P

SLOTS = 12
LOADS = 2
SECOND = 4
HELD = (13, 12)
EARLY = 4
MESH_IDS = pl.DeviceIdType.MESH


def plain(master_gate, second_gate, master_up, second_up, router_weight, router_gain):
    merged_gate = master_gate + second_gate.astype(jnp.float32)
    merged_up = master_up + second_up.astype(jnp.float32)
    narrow_gate, narrow_up = (merged_gate.astype(jnp.bfloat16), merged_up.astype(jnp.bfloat16))
    final_gate, final_up = (
        lax.all_to_all(narrow_gate, "shard", split_axis=2, concat_axis=1, tiled=True),
        lax.all_to_all(narrow_up, "shard", split_axis=2, concat_axis=1, tiled=True),
    )
    final_gate = jnp.transpose(final_gate, (0, 2, 1))
    final_up = jnp.transpose(final_up, (0, 2, 1))
    part_router = (router_weight * router_gain[:, None]).astype(jnp.bfloat16)
    row_router = lax.all_gather(part_router, "shard", axis=0, tiled=True)
    serve_router = lax.all_gather(row_router, "expert", axis=1, tiled=True)
    return (final_gate, final_up, serve_router)


def peers(me, n):
    half, quarter = n // 2, n // 4
    mine, place = me // half, me % half
    is_end = (place // quarter) == mine
    far_end = [(1 - mine) * (n - quarter) + i for i in range(quarter)]
    far_mid = [half - mine * quarter + i for i in range(quarter)]
    near = [mine * half + (place + i) % half for i in range(1, half)]
    return is_end, far_end, far_mid, near


def regroup_kernel(n, groups, mg, sg, mu, su, rw, gain, og, ou, orr, stash,
                   in_m, in_s, stage, rw_v, gain_v, r_part, r_all,
                   load_m, load_s, load_r, send, own, recv, r_send, r_recv, f_send, f_recv, known, crossed, all_known):
    experts, rows, inner = mg.shape
    part = inner // n
    r_cols = rw.shape[0]
    group, me = lax.axis_index("expert"), lax.axis_index("shard")
    is_end, far_end, far_mid, near = peers(me, n)
    half, quarter = n // 2, n // 4
    mine, x = me // half, me % quarter
    mirror_x = jnp.where(is_end, far_end[0], far_mid[0]) + x
    near_mid = half - (1 - mine) * quarter + x
    near_end = mine * (n - quarter)
    total = 2 * experts
    held = jnp.where(group % 2 == 0, HELD[0], HELD[1])
    other = [(group + i) % groups for i in range(1, groups)]
    masters, seconds, outs = (mg, mu), (sg, su), (og, ou)
    home = pl.ds(pl.multiple_of(me * rows, rows), rows)

    def loads(a, e):
        slot = e % LOADS
        return (
            pltpu.make_async_copy(masters[a].at[e], in_m.at[a, slot], load_m.at[a, slot]),
            pltpu.make_async_copy(seconds[a].at[e], in_s.at[a, slot], load_s.at[a, slot]),
        )

    def start_loads(a, e):
        for copy in loads(a, e):
            copy.start()

    def router_loads():
        return (
            pltpu.make_async_copy(rw, rw_v, load_r.at[0]),
            pltpu.make_async_copy(gain, gain_v, load_r.at[1]),
        )

    def block(a, e, device):
        src = pl.ds(pl.multiple_of(device * part, part), part)
        return stage.at[a, e % SLOTS, src, :], outs[a].at[e, :, home]

    def send_to(a, e, devices):
        for device in devices:
            src, dst = block(a, e, device)
            pltpu.make_async_remote_copy(
                src_ref=src, dst_ref=dst, send_sem=send.at[a, e % SLOTS], recv_sem=recv.at[a, e],
                device_id=(group, device), device_id_type=MESH_IDS,
            ).start()

    def seconds_of(a, e):
        return is_end & (2 * e + a >= total - SECOND)

    def start_sends(a, e, early=False):
        m = 2 * e + a

        @pl.when(~seconds_of(a, e))
        def _():
            send_to(a, e, far_end)

        for i, device in enumerate(far_mid):
            @pl.when(is_end | (x != i if early else m * quarter + i < total * quarter - held))
            def _():
                send_to(a, e, [device])

        send_to(a, e, near)
        src, dst = block(a, e, me)
        pltpu.make_async_copy(src, dst, own.at[a, e % SLOTS]).start()

    def wait_sends(a, e, blocks=n - 1):
        many = stage.at[a, e % SLOTS, pl.ds(0, blocks * part), :]
        pltpu.make_async_copy(many, many, send.at[a, e % SLOTS]).wait()
        src, dst = block(a, e, me)
        pltpu.make_async_copy(src, dst, own.at[a, e % SLOTS]).wait()

    def merge(a, e):
        for copy in loads(a, e):
            copy.wait()

        @pl.when(e >= SLOTS)
        def _():
            wait_sends(a, e - SLOTS)

        slot, into = e % LOADS, e % SLOTS
        for c in range(inner // 128):
            cols = slice(c * 128, (c + 1) * 128)
            merged = in_m[a, slot, :, cols] + in_s[a, slot, :, cols].astype(jnp.float32)
            stage[a, into, cols, :] = merged.T.astype(jnp.bfloat16)

        @pl.when(2 * e + a >= total - SECOND)
        def _():
            theirs = pl.ds(pl.multiple_of(far_end[0] * part, quarter * part), quarter * part)
            stash[2 * e + a - (total - SECOND)] = stage[a, into, theirs, :]

        @pl.when(e + LOADS < experts)
        def _():
            start_loads(a, e + LOADS)

    for a in range(2):
        start_loads(a, 0)
    for copy in router_loads():
        copy.start()
    for e in range(1, LOADS):
        for a in range(2):
            start_loads(a, e)

    barrier = pltpu.get_barrier_semaphore()

    def greet(group, device):
        pl.semaphore_signal(barrier, inc=1, device_id=(group, device), device_id_type=MESH_IDS)

    def tell(flag, group, device):
        pl.semaphore_signal(flag, inc=1, device_id=(group, device), device_id_type=MESH_IDS)

    @pl.when(is_end)
    def _():
        for device in far_end:
            greet(group, device)
        for i in range(1, quarter):
            greet(group, near_end + (x + i) % quarter)
        for g in other:
            greet(g, me)

    @pl.when(~is_end)
    def _():
        greet(group, mirror_x)
        pl.semaphore_wait(barrier, 1)
        for device in far_end:
            greet(group, device)
        for i in range(quarter):
            greet(group, near_end + (x + i) % quarter)

    def send_early(a, e):
        @pl.when(~is_end)
        def _():
            send_to(a, e, [mirror_x])

    r_rows = pl.ds(pl.multiple_of(group * r_cols, r_cols), r_cols)
    for m in range(EARLY):
        merge(m % 2, m // 2)
        if m == 0:
            for copy in router_loads():
                copy.wait()
            weight = (rw_v[...] * gain_v[...]).astype(jnp.bfloat16)
            r_part[...] = weight
            r_all[r_rows, home] = weight
            send_early(0, 0)
        if m == 1:
            @pl.when(is_end)
            def _():
                pl.semaphore_wait(barrier, n - 1 + len(other))
                tell(known, group, near_mid)
                for g in other:
                    tell(crossed, g, me)
        if m > 1:
            send_early((m - 1) % 2, (m - 1) // 2)
    send_early((EARLY - 1) % 2, (EARLY - 1) // 2)

    @pl.when(~is_end)
    def _():
        pl.semaphore_wait(known, 1)

    for m in range(EARLY):
        start_sends(m % 2, m // 2, early=True)

    def hand(src, dst, i, device):
        pltpu.make_async_remote_copy(
            src_ref=src, dst_ref=dst, send_sem=r_send.at[i], recv_sem=r_recv.at[i],
            device_id=(group, device), device_id_type=MESH_IDS,
        ).start()

    def wait_hands(sems, i, count):
        many = r_all.at[pl.ds(0, r_cols), pl.ds(0, count * rows)]
        pltpu.make_async_copy(many, many, sems.at[i]).wait()

    hand(r_part, r_all.at[r_rows, home], 0, mirror_x)
    for device in near:
        hand(r_part, r_all.at[r_rows, home], 1, device)

    merge(0, EARLY // 2)
    merge(1, EARLY // 2)
    start_sends(0, EARLY // 2)

    def step(e, carry):
        merge(0, e)
        start_sends(1, e - 1)
        merge(1, e)
        start_sends(0, e)
        return carry

    lax.fori_loop(EARLY // 2 + 1, experts, step, 0)

    start_sends(1, experts - 1)

    @pl.when(~is_end)
    def _():
        for i in range(total * quarter - max(HELD), total * quarter):
            m = i // quarter

            @pl.when(i >= total * quarter - held)
            def _():
                send_to(m % 2, m // 2, [far_mid[i % quarter]])

    wait_hands(r_recv, 0, 1)
    mirror = r_all.at[r_rows, pl.ds(pl.multiple_of(mirror_x * rows, rows), rows)]
    for device in near:
        hand(mirror, mirror, 2, device)
    wait_hands(r_send, 0, 1)
    for i in (1, 2):
        wait_hands(r_recv, i, len(near))
        wait_hands(r_send, i, len(near))
    @pl.when(is_end)
    def _():
        pl.semaphore_wait(crossed, len(other))
        tell(all_known, group, near_mid)

    @pl.when(~is_end)
    def _():
        pl.semaphore_wait(all_known, 1)

    for g in other:
        pltpu.make_async_remote_copy(
            src_ref=r_all.at[r_rows, :], dst_ref=r_all.at[r_rows, :], send_sem=f_send, recv_sem=f_recv,
            device_id=(g, me), device_id_type=MESH_IDS,
        ).start()
    many = r_all.at[pl.ds(0, (groups - 1) * r_cols), :]
    pltpu.make_async_copy(many, many, f_recv).wait()
    pltpu.make_async_copy(many, many, f_send).wait()
    for c in range(orr.shape[0] // 128):
        span = slice(c * 128, (c + 1) * 128)
        orr[span, :] = r_all[:, span].astype(jnp.float32).T.astype(jnp.bfloat16)

    def drain(e, carry):
        for a in range(2):
            @pl.when(seconds_of(a, e))
            def _():
                wait_sends(a, e, n - 1 - quarter)

            @pl.when(~seconds_of(a, e))
            def _():
                wait_sends(a, e)
        return carry

    lax.fori_loop(max(experts - SLOTS, 0), experts, drain, 0)

    def wait_recv(a, e, blocks):
        many = outs[a].at[e, :, pl.ds(0, blocks * rows)]
        pltpu.make_async_copy(many, many, recv.at[a, e]).wait()

    def arrive(e, carry):
        for a in range(2):
            @pl.when(seconds_of(a, e))
            def _():
                wait_recv(a, e, n - 1 - quarter)

            @pl.when(~seconds_of(a, e))
            def _():
                wait_recv(a, e, n - 1)
        return carry

    lax.fori_loop(0, experts, arrive, 0)


def second_kernel(n, stash, after, land, send, recv):
    group, me = lax.axis_index("expert"), lax.axis_index("shard")
    is_end, far_end, _, _ = peers(me, n)
    quarter = n // 4
    part, rows = stash.shape[1] // quarter, stash.shape[2]
    x = me % quarter
    barrier = pltpu.get_barrier_semaphore()

    @pl.when(is_end)
    def _():
        for device in far_end:
            pl.semaphore_signal(barrier, inc=1, device_id=(group, device), device_id_type=MESH_IDS)
        pl.semaphore_wait(barrier, quarter)
        for i in range(quarter * SECOND):
            to, m = i // SECOND, i % SECOND
            pltpu.make_async_remote_copy(
                src_ref=stash.at[m, pl.ds(to * part, part), :],
                dst_ref=land.at[m, :, pl.ds(pl.multiple_of(x * rows, rows), rows)],
                send_sem=send, recv_sem=recv,
                device_id=(group, far_end[to]), device_id_type=MESH_IDS,
            ).start()
        pltpu.make_async_copy(land, land, recv).wait()
        pltpu.make_async_copy(stash, stash, send).wait()


def second(n, stash, after):
    _, span, rows = stash.shape
    quarter = n // 4
    anywhere = pl.BlockSpec(memory_space=pl.ANY)
    return pl.pallas_call(
        functools.partial(second_kernel, n),
        out_shape=pltpu.VMEM((SECOND, span // quarter, quarter * rows), stash.dtype),
        in_specs=[anywhere, anywhere],
        out_specs=anywhere,
        scratch_shapes=[pltpu.SemaphoreType.DMA, pltpu.SemaphoreType.DMA],
        compiler_params=pltpu.CompilerParams(
            collective_id=1, has_side_effects=True, vmem_limit_bytes=1024 * 1024,
        ),
        name="second",
    )(stash, after)


def fill_kernel(n, gate, up, land, og, ou, done):
    me = lax.axis_index("shard")
    is_end, _, _, _ = peers(me, n)
    half, quarter = n // 2, n // 4
    experts, width = gate.shape[0], land.shape[2]
    spot = pl.ds(pl.multiple_of((1 - me // half) * (n - quarter) * (width // quarter), width), width)

    @pl.when(is_end)
    def _():
        copies = []
        for i in range(SECOND):
            m = 2 * experts - SECOND + i
            copies.append(pltpu.make_async_copy(land.at[i], (og, ou)[m % 2].at[m // 2, :, spot], done.at[i]))
        for copy in copies:
            copy.start()
        for copy in copies:
            copy.wait()


def fill(n, gate, up, land):
    anywhere = pl.BlockSpec(memory_space=pl.ANY)
    return pl.pallas_call(
        functools.partial(fill_kernel, n),
        out_shape=tuple(pltpu.HBM(x.shape, x.dtype) for x in (gate, up)),
        in_specs=[anywhere] * 3,
        out_specs=(anywhere,) * 2,
        scratch_shapes=[pltpu.SemaphoreType.DMA((SECOND,))],
        input_output_aliases={0: 0, 1: 1},
        compiler_params=pltpu.CompilerParams(vmem_limit_bytes=1024 * 1024),
        name="fill",
    )(gate, up, land)


PIECES = 4


def put_kernel(gate, up, router, og, ou, orr, after, done, done_router):
    size = gate.shape[0] // PIECES
    copies = [
        pltpu.make_async_copy(src.at[pl.ds(i * size, size)], dst.at[pl.ds(i * size, size)], done.at[a, i])
        for i in range(PIECES)
        for a, (src, dst) in enumerate(((gate, og), (up, ou)))
    ]
    copies.append(pltpu.make_async_copy(router, orr, done_router))
    for copy in copies:
        copy.start()
    for copy in copies:
        copy.wait()


def put(*held):
    anywhere = pl.BlockSpec(memory_space=pl.ANY)
    return pl.pallas_call(
        put_kernel,
        out_shape=tuple(pltpu.HBM(x.shape, x.dtype) for x in held) + (pltpu.VMEM((8, 128), jnp.float32),),
        in_specs=[anywhere] * len(held),
        out_specs=(anywhere,) * (len(held) + 1),
        scratch_shapes=[pltpu.SemaphoreType.DMA((2, PIECES)), pltpu.SemaphoreType.DMA],
        compiler_params=pltpu.CompilerParams(vmem_limit_bytes=1024 * 1024),
        name="put",
    )(*held)


def fused(n, groups, master_gate, second_gate, master_up, second_up, router_weight, router_gain):
    experts, rows, inner = master_gate.shape
    r_cols = router_weight.shape[1]
    final = (experts, inner // n, rows * n)
    anywhere = pl.BlockSpec(memory_space=pl.ANY)
    dma, regular = pltpu.SemaphoreType.DMA, pltpu.SemaphoreType.REGULAR
    *held, stash = pl.pallas_call(
        functools.partial(regroup_kernel, n, groups),
        out_shape=(
            pltpu.VMEM(final, jnp.bfloat16),
            pltpu.VMEM(final, jnp.bfloat16),
            jax.ShapeDtypeStruct((rows * n, r_cols * groups), jnp.bfloat16),
            pltpu.VMEM((SECOND, inner // 4, rows), jnp.bfloat16),
        ),
        in_specs=[anywhere] * 6,
        out_specs=(anywhere, anywhere, pl.BlockSpec(memory_space=pltpu.VMEM), pl.BlockSpec(memory_space=pltpu.VMEM)),
        scratch_shapes=[
            pltpu.VMEM((2, LOADS, rows, inner), jnp.float32),
            pltpu.VMEM((2, LOADS, rows, inner), jnp.bfloat16),
            pltpu.VMEM((2, SLOTS, inner, rows), jnp.bfloat16),
            pltpu.VMEM((r_cols, rows), jnp.float32),
            pltpu.VMEM((1, rows), jnp.float32),
            pltpu.VMEM((r_cols, rows), jnp.bfloat16),
            pltpu.VMEM((r_cols * groups, rows * n), jnp.bfloat16),
            dma((2, LOADS)), dma((2, LOADS)), dma((2,)),
            dma((2, SLOTS)), dma((2, SLOTS)), dma((2, experts)),
            dma((3,)), dma((3,)), dma, dma,
            regular, regular, regular,
        ],
        compiler_params=pltpu.CompilerParams(
            collective_id=0, has_side_effects=True, vmem_limit_bytes=24 * 1024 * 1024,
        ),
        name="regroup",
    )(
        master_gate, second_gate, master_up, second_up,
        pltpu.with_memory_space_constraint(router_weight.T, pltpu.HBM),
        pltpu.with_memory_space_constraint(router_gain[None, :], pltpu.HBM),
    )
    gate, up, router, after = put(*held)
    return *fill(n, gate, up, second(n, stash, after)), router


def solution(mesh):
    n, groups = mesh.shape["shard"], mesh.shape["expert"]

    def shards(*args):
        experts, rows, inner = args[0].shape
        r_cols = args[4].shape[1]
        fits = (
            n % 4 == 0 and groups > 1 and rows % 128 == 0 and inner % 128 == 0
            and (inner // n) % 16 == 0 and r_cols % 16 == 0 and experts % PIECES == 0 and experts > max(SLOTS, LOADS, EARLY) and 2 * SLOTS * (n // 4) > max(HELD) + n // 2
        )
        return fused(n, groups, *args) if fits else plain(*args)

    in_specs = (
        P("expert", "shard", None),
        P("expert", "shard", None),
        P("expert", "shard", None),
        P("expert", "shard", None),
        P("shard", "expert"),
        P("shard"),
    )
    out_specs = (P("expert", "shard", None), P("expert", "shard", None), P())
    return jax.shard_map(shards, mesh=mesh, in_specs=in_specs, out_specs=out_specs, check_vma=False)
```

```python
import functools

import jax
import jax.numpy as jnp
from jax import lax
from jax.experimental import pallas as pl
from jax.experimental.pallas import tpu as pltpu
from jax.sharding import PartitionSpec as P

SLOTS = 12
LOADS = 2
ENDS = 6
MIDS = 1
HELD = (13, 12)
EARLY = 8
MESH_IDS = pl.DeviceIdType.MESH


def plain(master_gate, second_gate, master_up, second_up, router_weight, router_gain):
    merged_gate = master_gate + second_gate.astype(jnp.float32)
    merged_up = master_up + second_up.astype(jnp.float32)
    narrow_gate, narrow_up = (merged_gate.astype(jnp.bfloat16), merged_up.astype(jnp.bfloat16))
    final_gate, final_up = (
        lax.all_to_all(narrow_gate, "shard", split_axis=2, concat_axis=1, tiled=True),
        lax.all_to_all(narrow_up, "shard", split_axis=2, concat_axis=1, tiled=True),
    )
    final_gate = jnp.transpose(final_gate, (0, 2, 1))
    final_up = jnp.transpose(final_up, (0, 2, 1))
    part_router = (router_weight * router_gain[:, None]).astype(jnp.bfloat16)
    row_router = lax.all_gather(part_router, "shard", axis=0, tiled=True)
    serve_router = lax.all_gather(row_router, "expert", axis=1, tiled=True)
    return (final_gate, final_up, serve_router)


def peers(me, n):
    half, quarter = n // 2, n // 4
    mine, place = me // half, me % half
    is_end = (place // quarter) == mine
    far_end = [(1 - mine) * (n - quarter) + i for i in range(quarter)]
    far_mid = [half - mine * quarter + i for i in range(quarter)]
    near = [mine * half + (place + i) % half for i in range(1, half)]
    return is_end, far_end, far_mid, near


def regroup_kernel(n, groups, mg, sg, mu, su, rw, gain, og, ou, orr, stash,
                   in_m, in_s, stage, rw_v, gain_v, r_part, r_all,
                   load_m, load_s, load_r, send, own, recv, r_send, r_recv, f_send, f_recv, known, crossed, all_known):
    experts, rows, inner = mg.shape
    part = inner // n
    r_cols = rw.shape[0]
    group, me = lax.axis_index("expert"), lax.axis_index("shard")
    is_end, far_end, far_mid, near = peers(me, n)
    half, quarter = n // 2, n // 4
    mine, x = me // half, me % quarter
    mirror_x = jnp.where(is_end, far_end[0], far_mid[0]) + x
    near_mid = half - (1 - mine) * quarter + x
    near_end = mine * (n - quarter)
    total = 2 * experts
    held = jnp.where(group % 2 == 0, HELD[0], HELD[1])
    other = [(group + i) % groups for i in range(1, groups)]
    masters, seconds, outs = (mg, mu), (sg, su), (og, ou)
    home = pl.ds(pl.multiple_of(me * rows, rows), rows)

    def loads(a, e):
        slot = e % LOADS
        return (
            pltpu.make_async_copy(masters[a].at[e], in_m.at[a, slot], load_m.at[a, slot]),
            pltpu.make_async_copy(seconds[a].at[e], in_s.at[a, slot], load_s.at[a, slot]),
        )

    def start_loads(a, e):
        for copy in loads(a, e):
            copy.start()

    def router_loads():
        return (
            pltpu.make_async_copy(rw, rw_v, load_r.at[0]),
            pltpu.make_async_copy(gain, gain_v, load_r.at[1]),
        )

    def block(a, e, device):
        src = pl.ds(pl.multiple_of(device * part, part), part)
        return stage.at[a, e % SLOTS, src, :], outs[a].at[e, :, home]

    def send_to(a, e, devices):
        for device in devices:
            src, dst = block(a, e, device)
            pltpu.make_async_remote_copy(
                src_ref=src, dst_ref=dst, send_sem=send.at[a, e % SLOTS], recv_sem=recv.at[a, e],
                device_id=(group, device), device_id_type=MESH_IDS,
            ).start()

    def seconds_of(a, e):
        return 2 * e + a >= total - jnp.where(is_end, ENDS, MIDS)

    def start_sends(a, e, early=False):
        m = 2 * e + a

        @pl.when(~is_end | (m < total - ENDS))
        def _():
            send_to(a, e, far_end)

        for i, device in enumerate(far_mid):
            @pl.when(is_end | (x != i if early else m * quarter + i < (total - MIDS) * quarter - held))
            def _():
                send_to(a, e, [device])

        send_to(a, e, near)
        src, dst = block(a, e, me)
        pltpu.make_async_copy(src, dst, own.at[a, e % SLOTS]).start()

    def wait_sends(a, e, blocks=n - 1):
        many = stage.at[a, e % SLOTS, pl.ds(0, blocks * part), :]
        pltpu.make_async_copy(many, many, send.at[a, e % SLOTS]).wait()
        src, dst = block(a, e, me)
        pltpu.make_async_copy(src, dst, own.at[a, e % SLOTS]).wait()

    def merge(a, e):
        for copy in loads(a, e):
            copy.wait()

        @pl.when(e >= SLOTS)
        def _():
            wait_sends(a, e - SLOTS)

        slot, into = e % LOADS, e % SLOTS
        for c in range(inner // 128):
            cols = slice(c * 128, (c + 1) * 128)
            merged = in_m[a, slot, :, cols] + in_s[a, slot, :, cols].astype(jnp.float32)
            stage[a, into, cols, :] = merged.T.astype(jnp.bfloat16)

        @pl.when(2 * e + a >= total - ENDS)
        def _():
            theirs = pl.ds(pl.multiple_of(jnp.where(is_end, far_end[0], far_mid[0]) * part, quarter * part), quarter * part)
            stash[2 * e + a - (total - ENDS)] = stage[a, into, theirs, :]

        @pl.when(e + LOADS < experts)
        def _():
            start_loads(a, e + LOADS)

    for a in range(2):
        start_loads(a, 0)
    for copy in router_loads():
        copy.start()
    for e in range(1, LOADS):
        for a in range(2):
            start_loads(a, e)

    barrier = pltpu.get_barrier_semaphore()

    def greet(group, device):
        pl.semaphore_signal(barrier, inc=1, device_id=(group, device), device_id_type=MESH_IDS)

    def tell(flag, group, device):
        pl.semaphore_signal(flag, inc=1, device_id=(group, device), device_id_type=MESH_IDS)

    @pl.when(is_end)
    def _():
        for device in far_end:
            greet(group, device)
        for i in range(1, quarter):
            greet(group, near_end + (x + i) % quarter)
        for g in other:
            greet(g, me)

    @pl.when(~is_end)
    def _():
        greet(group, mirror_x)
        pl.semaphore_wait(barrier, 1)
        for device in far_end:
            greet(group, device)
        for i in range(quarter):
            greet(group, near_end + (x + i) % quarter)

    def send_early(a, e):
        @pl.when(~is_end)
        def _():
            send_to(a, e, [mirror_x])

    r_rows = pl.ds(pl.multiple_of(group * r_cols, r_cols), r_cols)
    for m in range(EARLY):
        merge(m % 2, m // 2)
        if m == 0:
            for copy in router_loads():
                copy.wait()
            weight = (rw_v[...] * gain_v[...]).astype(jnp.bfloat16)
            r_part[...] = weight
            r_all[r_rows, home] = weight
            send_early(0, 0)
        if m == 1:
            @pl.when(is_end)
            def _():
                pl.semaphore_wait(barrier, n - 1 + len(other))
                tell(known, group, near_mid)
                for g in other:
                    tell(crossed, g, me)
        if m > 1:
            send_early((m - 1) % 2, (m - 1) // 2)
    send_early((EARLY - 1) % 2, (EARLY - 1) // 2)

    @pl.when(~is_end)
    def _():
        pl.semaphore_wait(known, 1)

    for m in range(EARLY):
        start_sends(m % 2, m // 2, early=True)

    def hand(src, dst, i, device):
        pltpu.make_async_remote_copy(
            src_ref=src, dst_ref=dst, send_sem=r_send.at[i], recv_sem=r_recv.at[i],
            device_id=(group, device), device_id_type=MESH_IDS,
        ).start()

    def wait_hands(sems, i, count):
        many = r_all.at[pl.ds(0, r_cols), pl.ds(0, count * rows)]
        pltpu.make_async_copy(many, many, sems.at[i]).wait()

    hand(r_part, r_all.at[r_rows, home], 0, mirror_x)
    for device in near:
        hand(r_part, r_all.at[r_rows, home], 1, device)

    merge(0, EARLY // 2)
    merge(1, EARLY // 2)
    start_sends(0, EARLY // 2)

    def step(e, carry):
        merge(0, e)
        start_sends(1, e - 1)
        merge(1, e)
        start_sends(0, e)
        return carry

    lax.fori_loop(EARLY // 2 + 1, experts, step, 0)

    start_sends(1, experts - 1)

    @pl.when(~is_end)
    def _():
        for i in range((total - MIDS) * quarter - max(HELD), (total - MIDS) * quarter):
            m = i // quarter

            @pl.when(i >= (total - MIDS) * quarter - held)
            def _():
                send_to(m % 2, m // 2, [far_mid[i % quarter]])

    wait_hands(r_recv, 0, 1)
    mirror = r_all.at[r_rows, pl.ds(pl.multiple_of(mirror_x * rows, rows), rows)]
    for device in near:
        hand(mirror, mirror, 2, device)
    wait_hands(r_send, 0, 1)
    for i in (1, 2):
        wait_hands(r_recv, i, len(near))
        wait_hands(r_send, i, len(near))
    @pl.when(is_end)
    def _():
        pl.semaphore_wait(crossed, len(other))
        tell(all_known, group, near_mid)

    @pl.when(~is_end)
    def _():
        pl.semaphore_wait(all_known, 1)

    for g in other:
        pltpu.make_async_remote_copy(
            src_ref=r_all.at[r_rows, :], dst_ref=r_all.at[r_rows, :], send_sem=f_send, recv_sem=f_recv,
            device_id=(g, me), device_id_type=MESH_IDS,
        ).start()
    many = r_all.at[pl.ds(0, (groups - 1) * r_cols), :]
    pltpu.make_async_copy(many, many, f_recv).wait()
    pltpu.make_async_copy(many, many, f_send).wait()
    for c in range(orr.shape[0] // 128):
        span = slice(c * 128, (c + 1) * 128)
        orr[span, :] = r_all[:, span].astype(jnp.float32).T.astype(jnp.bfloat16)

    def drain(e, carry):
        for a in range(2):
            @pl.when(seconds_of(a, e))
            def _():
                wait_sends(a, e, n - 1 - quarter)

            @pl.when(~seconds_of(a, e))
            def _():
                wait_sends(a, e)
        return carry

    lax.fori_loop(max(experts - SLOTS, 0), experts, drain, 0)

    def wait_recv(a, e, blocks):
        many = outs[a].at[e, :, pl.ds(0, blocks * rows)]
        pltpu.make_async_copy(many, many, recv.at[a, e]).wait()

    def arrive(e, carry):
        for a in range(2):
            @pl.when(seconds_of(a, e))
            def _():
                wait_recv(a, e, n - 1 - quarter)

            @pl.when(~seconds_of(a, e))
            def _():
                wait_recv(a, e, n - 1)
        return carry

    lax.fori_loop(0, experts, arrive, 0)


def second_kernel(n, stash, after, land, send, recv):
    group, me = lax.axis_index("expert"), lax.axis_index("shard")
    is_end, far_end, far_mid, _ = peers(me, n)
    quarter = n // 4
    part, rows = stash.shape[1] // quarter, stash.shape[2]
    x = me % quarter
    barrier = pltpu.get_barrier_semaphore()
    for i in range(quarter):
        device = jnp.where(is_end, far_end[i], far_mid[i])
        pl.semaphore_signal(barrier, inc=1, device_id=(group, device), device_id_type=MESH_IDS)
    pl.semaphore_wait(barrier, quarter)

    def exchange(first, base, start):
        for i in range(quarter):
            to = (start + i) % quarter
            for m in range(first, ENDS):
                pltpu.make_async_remote_copy(
                    src_ref=stash.at[m, pl.ds(pl.multiple_of(to * part, part), part), :],
                    dst_ref=land.at[m, :, pl.ds(pl.multiple_of(x * rows, rows), rows)],
                    send_sem=send, recv_sem=recv, device_id=(group, base + to), device_id_type=MESH_IDS,
                ).start()
        got, sent = land.at[pl.ds(first, ENDS - first)], stash.at[pl.ds(first, ENDS - first)]
        pltpu.make_async_copy(got, got, recv).wait()
        pltpu.make_async_copy(sent, sent, send).wait()

    @pl.when(is_end)
    def _():
        exchange(0, far_end[0], 0)

    @pl.when(~is_end)
    def _():
        exchange(ENDS - MIDS, far_mid[0], x + 1)


def second(n, stash, after):
    _, span, rows = stash.shape
    quarter = n // 4
    anywhere = pl.BlockSpec(memory_space=pl.ANY)
    return pl.pallas_call(
        functools.partial(second_kernel, n),
        out_shape=pltpu.VMEM((ENDS, span // quarter, quarter * rows), stash.dtype),
        in_specs=[anywhere, anywhere],
        out_specs=anywhere,
        scratch_shapes=[pltpu.SemaphoreType.DMA, pltpu.SemaphoreType.DMA],
        compiler_params=pltpu.CompilerParams(
            collective_id=1, has_side_effects=True, vmem_limit_bytes=1024 * 1024,
        ),
        name="second",
    )(stash, after)


def fill_kernel(n, gate, up, land, og, ou, done):
    me = lax.axis_index("shard")
    is_end, far_end, far_mid, _ = peers(me, n)
    experts, width = gate.shape[0], land.shape[2]
    rows = width // (n // 4)

    def place(first, base):
        spot = pl.ds(pl.multiple_of(base * rows, width), width)
        copies = []
        for i in range(first, ENDS):
            m = 2 * experts - ENDS + i
            copies.append(pltpu.make_async_copy(land.at[i], (og, ou)[m % 2].at[m // 2, :, spot], done.at[i]))
        for copy in copies:
            copy.start()
        for copy in copies:
            copy.wait()

    @pl.when(is_end)
    def _():
        place(0, far_end[0])

    @pl.when(~is_end)
    def _():
        place(ENDS - MIDS, far_mid[0])


def fill(n, gate, up, land):
    anywhere = pl.BlockSpec(memory_space=pl.ANY)
    return pl.pallas_call(
        functools.partial(fill_kernel, n),
        out_shape=tuple(pltpu.HBM(x.shape, x.dtype) for x in (gate, up)),
        in_specs=[anywhere] * 3,
        out_specs=(anywhere,) * 2,
        scratch_shapes=[pltpu.SemaphoreType.DMA((ENDS,))],
        input_output_aliases={0: 0, 1: 1},
        compiler_params=pltpu.CompilerParams(vmem_limit_bytes=1024 * 1024),
        name="fill",
    )(gate, up, land)


PIECES = 4


def put_kernel(gate, up, router, og, ou, orr, after, done, done_router):
    size = gate.shape[0] // PIECES
    copies = [
        pltpu.make_async_copy(src.at[pl.ds(i * size, size)], dst.at[pl.ds(i * size, size)], done.at[a, i])
        for i in range(PIECES)
        for a, (src, dst) in enumerate(((gate, og), (up, ou)))
    ]
    copies.append(pltpu.make_async_copy(router, orr, done_router))
    for copy in copies:
        copy.start()
    for copy in copies:
        copy.wait()


def put(*held):
    anywhere = pl.BlockSpec(memory_space=pl.ANY)
    return pl.pallas_call(
        put_kernel,
        out_shape=tuple(pltpu.HBM(x.shape, x.dtype) for x in held) + (pltpu.VMEM((8, 128), jnp.float32),),
        in_specs=[anywhere] * len(held),
        out_specs=(anywhere,) * (len(held) + 1),
        scratch_shapes=[pltpu.SemaphoreType.DMA((2, PIECES)), pltpu.SemaphoreType.DMA],
        compiler_params=pltpu.CompilerParams(vmem_limit_bytes=1024 * 1024),
        name="put",
    )(*held)


def fused(n, groups, master_gate, second_gate, master_up, second_up, router_weight, router_gain):
    experts, rows, inner = master_gate.shape
    r_cols = router_weight.shape[1]
    final = (experts, inner // n, rows * n)
    anywhere = pl.BlockSpec(memory_space=pl.ANY)
    dma, regular = pltpu.SemaphoreType.DMA, pltpu.SemaphoreType.REGULAR
    *held, stash = pl.pallas_call(
        functools.partial(regroup_kernel, n, groups),
        out_shape=(
            pltpu.VMEM(final, jnp.bfloat16),
            pltpu.VMEM(final, jnp.bfloat16),
            jax.ShapeDtypeStruct((rows * n, r_cols * groups), jnp.bfloat16),
            pltpu.VMEM((ENDS, inner // 4, rows), jnp.bfloat16),
        ),
        in_specs=[anywhere] * 6,
        out_specs=(anywhere, anywhere, pl.BlockSpec(memory_space=pltpu.VMEM), pl.BlockSpec(memory_space=pltpu.VMEM)),
        scratch_shapes=[
            pltpu.VMEM((2, LOADS, rows, inner), jnp.float32),
            pltpu.VMEM((2, LOADS, rows, inner), jnp.bfloat16),
            pltpu.VMEM((2, SLOTS, inner, rows), jnp.bfloat16),
            pltpu.VMEM((r_cols, rows), jnp.float32),
            pltpu.VMEM((1, rows), jnp.float32),
            pltpu.VMEM((r_cols, rows), jnp.bfloat16),
            pltpu.VMEM((r_cols * groups, rows * n), jnp.bfloat16),
            dma((2, LOADS)), dma((2, LOADS)), dma((2,)),
            dma((2, SLOTS)), dma((2, SLOTS)), dma((2, experts)),
            dma((3,)), dma((3,)), dma, dma,
            regular, regular, regular,
        ],
        compiler_params=pltpu.CompilerParams(
            collective_id=0, has_side_effects=True, vmem_limit_bytes=24 * 1024 * 1024,
        ),
        name="regroup",
    )(
        master_gate, second_gate, master_up, second_up,
        pltpu.with_memory_space_constraint(router_weight.T, pltpu.HBM),
        pltpu.with_memory_space_constraint(router_gain[None, :], pltpu.HBM),
    )
    gate, up, router, after = put(*held)
    return *fill(n, gate, up, second(n, stash, after)), router


def solution(mesh):
    n, groups = mesh.shape["shard"], mesh.shape["expert"]

    def shards(*args):
        experts, rows, inner = args[0].shape
        r_cols = args[4].shape[1]
        fits = (
            n % 4 == 0 and groups > 1 and rows % 128 == 0 and inner % 128 == 0
            and (inner // n) % 16 == 0 and r_cols % 16 == 0 and experts % PIECES == 0 and experts > max(SLOTS, LOADS, EARLY) and 2 * SLOTS * (n // 4) > max(HELD) + (MIDS + 2) * (n // 4) and ENDS >= MIDS
        )
        return fused(n, groups, *args) if fits else plain(*args)

    in_specs = (
        P("expert", "shard", None),
        P("expert", "shard", None),
        P("expert", "shard", None),
        P("expert", "shard", None),
        P("shard", "expert"),
        P("shard"),
    )
    out_specs = (P("expert", "shard", None), P("expert", "shard", None), P())
    return jax.shard_map(shards, mesh=mesh, in_specs=in_specs, out_specs=out_specs, check_vma=False)
```

```python
import functools

import jax
import jax.numpy as jnp
from jax import lax
from jax.experimental import pallas as pl
from jax.experimental.pallas import tpu as pltpu
from jax.sharding import PartitionSpec as P

SLOTS = 12
LOADS = 2
ENDS = 6
MIDS = 1
HELD = (14, 12)
EARLY = 8
MESH_IDS = pl.DeviceIdType.MESH


def plain(master_gate, second_gate, master_up, second_up, router_weight, router_gain):
    merged_gate = master_gate + second_gate.astype(jnp.float32)
    merged_up = master_up + second_up.astype(jnp.float32)
    narrow_gate, narrow_up = (merged_gate.astype(jnp.bfloat16), merged_up.astype(jnp.bfloat16))
    final_gate, final_up = (
        lax.all_to_all(narrow_gate, "shard", split_axis=2, concat_axis=1, tiled=True),
        lax.all_to_all(narrow_up, "shard", split_axis=2, concat_axis=1, tiled=True),
    )
    final_gate = jnp.transpose(final_gate, (0, 2, 1))
    final_up = jnp.transpose(final_up, (0, 2, 1))
    part_router = (router_weight * router_gain[:, None]).astype(jnp.bfloat16)
    row_router = lax.all_gather(part_router, "shard", axis=0, tiled=True)
    serve_router = lax.all_gather(row_router, "expert", axis=1, tiled=True)
    return (final_gate, final_up, serve_router)


def peers(me, n):
    half, quarter = n // 2, n // 4
    mine, place = me // half, me % half
    is_end = (place // quarter) == mine
    far_end = [(1 - mine) * (n - quarter) + i for i in range(quarter)]
    far_mid = [half - mine * quarter + i for i in range(quarter)]
    near = [mine * half + (place + i) % half for i in range(1, half)]
    return is_end, far_end, far_mid, near


def late_pairs(n):
    blocks = max(MIDS * (n // 4) + max(HELD), ENDS * (n // 4))
    return -(-blocks // n)


def regroup_kernel(n, groups, mg, sg, mu, su, rw, gain, og, ou, orr, stash,
                   in_m, in_s, stage, rw_v, gain_v, r_part, r_all,
                   load_m, load_s, load_r, send, own, recv, r_send, r_recv, f_send, f_recv, known, crossed, all_known):
    experts, rows, inner = mg.shape
    part = inner // n
    r_cols = rw.shape[0]
    group, me = lax.axis_index("expert"), lax.axis_index("shard")
    is_end, far_end, far_mid, near = peers(me, n)
    half, quarter = n // 2, n // 4
    mine, x = me // half, me % quarter
    mirror_x = jnp.where(is_end, far_end[0], far_mid[0]) + x
    near_mid = half - (1 - mine) * quarter + x
    near_end = mine * (n - quarter)
    total = 2 * experts
    held = jnp.where(group % 2 == 0, HELD[0], HELD[1])
    other = [(group + i) % groups for i in range(1, groups)]
    masters, seconds, outs = (mg, mu), (sg, su), (og, ou)
    home = pl.ds(pl.multiple_of(me * rows, rows), rows)

    def loads(a, e):
        slot = e % LOADS
        return (
            pltpu.make_async_copy(masters[a].at[e], in_m.at[a, slot], load_m.at[a, slot]),
            pltpu.make_async_copy(seconds[a].at[e], in_s.at[a, slot], load_s.at[a, slot]),
        )

    def start_loads(a, e):
        for copy in loads(a, e):
            copy.start()

    def router_loads():
        return (
            pltpu.make_async_copy(rw, rw_v, load_r.at[0]),
            pltpu.make_async_copy(gain, gain_v, load_r.at[1]),
        )

    def block(a, e, count, device):
        src = pl.ds(pl.multiple_of(device * part, part), part)
        return stage.at[a, pl.ds(e % SLOTS, count), src, :], outs[a].at[pl.ds(e, count), :, home]

    def send_to(a, e, count, devices):
        for device in devices:
            src, dst = block(a, e, count, device)
            pltpu.make_async_remote_copy(
                src_ref=src, dst_ref=dst, send_sem=send.at[a, e // 2 % (SLOTS // 2)], recv_sem=recv.at[a, e // 2],
                device_id=(group, device), device_id_type=MESH_IDS,
            ).start()

    def own_copy(a, p):
        src, dst = block(a, 2 * p, 2, me)
        return pltpu.make_async_copy(src, dst, own.at[a, p % (SLOTS // 2)])

    def send_pair(a, p):
        send_to(a, 2 * p, 2, far_end + far_mid + near)
        own_copy(a, p).start()

    def start_sends(a, e, early=False):
        m = 2 * e + a

        @pl.when(~is_end | (m < total - ENDS))
        def _():
            send_to(a, e, 1, far_end)

        for i, device in enumerate(far_mid):
            @pl.when(is_end | (x != i if early else m * quarter + i < (total - MIDS) * quarter - held))
            def _():
                send_to(a, e, 1, [device])

        send_to(a, e, 1, near)

    def send_singles(a, p, early=False):
        for e in (2 * p, 2 * p + 1):
            start_sends(a, e, early)
        own_copy(a, p).start()

    def by_left_out(a, p, wait):
        first = total - jnp.where(is_end, ENDS, MIDS)
        for left_out, is_it in enumerate((
            4 * p + a + 2 < first, (4 * p + a < first) & (4 * p + a + 2 >= first), 4 * p + a >= first,
        )):
            @pl.when(is_it)
            def _():
                wait(n - 1 - left_out * quarter // 2)

    def wait_sends(a, p, blocks=n - 1):
        many = stage.at[a, pl.ds(2 * p % SLOTS, 2), pl.ds(0, blocks * part), :]
        pltpu.make_async_copy(many, many, send.at[a, p % (SLOTS // 2)]).wait()
        own_copy(a, p).wait()

    def merge(a, e):
        for copy in loads(a, e):
            copy.wait()

        @pl.when((e >= SLOTS) & (e % 2 == 0))
        def _():
            wait_sends(a, e // 2 - SLOTS // 2)

        slot, into = e % LOADS, e % SLOTS
        for c in range(inner // 128):
            cols = slice(c * 128, (c + 1) * 128)
            merged = in_m[a, slot, :, cols] + in_s[a, slot, :, cols].astype(jnp.float32)
            stage[a, into, cols, :] = merged.T.astype(jnp.bfloat16)

        @pl.when(2 * e + a >= total - ENDS)
        def _():
            theirs = pl.ds(pl.multiple_of(jnp.where(is_end, far_end[0], far_mid[0]) * part, quarter * part), quarter * part)
            stash[2 * e + a - (total - ENDS)] = stage[a, into, theirs, :]

        @pl.when(e + LOADS < experts)
        def _():
            start_loads(a, e + LOADS)

    for a in range(2):
        start_loads(a, 0)
    for copy in router_loads():
        copy.start()
    for e in range(1, LOADS):
        for a in range(2):
            start_loads(a, e)

    barrier = pltpu.get_barrier_semaphore()

    def greet(group, device):
        pl.semaphore_signal(barrier, inc=1, device_id=(group, device), device_id_type=MESH_IDS)

    def tell(flag, group, device):
        pl.semaphore_signal(flag, inc=1, device_id=(group, device), device_id_type=MESH_IDS)

    @pl.when(is_end)
    def _():
        for device in far_end:
            greet(group, device)
        for i in range(1, quarter):
            greet(group, near_end + (x + i) % quarter)
        for g in other:
            greet(g, me)

    @pl.when(~is_end)
    def _():
        greet(group, mirror_x)
        pl.semaphore_wait(barrier, 1)
        for device in far_end:
            greet(group, device)
        for i in range(quarter):
            greet(group, near_end + (x + i) % quarter)

    def send_early(a, e):
        @pl.when(~is_end)
        def _():
            send_to(a, e, 1, [mirror_x])

    r_rows = pl.ds(pl.multiple_of(group * r_cols, r_cols), r_cols)
    for m in range(EARLY):
        merge(m % 2, m // 2)
        if m == 0:
            for copy in router_loads():
                copy.wait()
            weight = (rw_v[...] * gain_v[...]).astype(jnp.bfloat16)
            r_part[...] = weight
            r_all[r_rows, home] = weight
            send_early(0, 0)
        if m == 1:
            @pl.when(is_end)
            def _():
                pl.semaphore_wait(barrier, n - 1 + len(other))
                tell(known, group, near_mid)
                for g in other:
                    tell(crossed, g, me)
        if m > 1:
            send_early((m - 1) % 2, (m - 1) // 2)
    send_early((EARLY - 1) % 2, (EARLY - 1) // 2)

    @pl.when(~is_end)
    def _():
        pl.semaphore_wait(known, 1)

    for p in range(EARLY // 4):
        for a in range(2):
            send_singles(a, p, early=True)

    def hand(src, dst, i, device):
        pltpu.make_async_remote_copy(
            src_ref=src, dst_ref=dst, send_sem=r_send.at[i], recv_sem=r_recv.at[i],
            device_id=(group, device), device_id_type=MESH_IDS,
        ).start()

    def wait_hands(sems, i, count):
        many = r_all.at[pl.ds(0, r_cols), pl.ds(0, count * rows)]
        pltpu.make_async_copy(many, many, sems.at[i]).wait()

    hand(r_part, r_all.at[r_rows, home], 0, mirror_x)
    for device in near:
        hand(r_part, r_all.at[r_rows, home], 1, device)

    def merge_pair(a, p):
        for e in (2 * p, 2 * p + 1):
            merge(a, e)

    pairs, late = experts // 2, late_pairs(n)

    def step(p, carry):
        merge_pair(0, p)

        @pl.when(p > EARLY // 4)
        def _():
            send_pair(1, p - 1)

        merge_pair(1, p)
        send_pair(0, p)
        return carry

    lax.fori_loop(EARLY // 4, pairs - late, step, 0)
    send_pair(1, pairs - late - 1)

    def late_step(p, carry):
        merge_pair(0, p)
        merge_pair(1, p)
        send_singles(0, p)
        send_singles(1, p)
        return carry

    lax.fori_loop(pairs - late, pairs, late_step, 0)

    @pl.when(~is_end)
    def _():
        for i in range((total - MIDS) * quarter - max(HELD), (total - MIDS) * quarter):
            m = i // quarter

            @pl.when(i >= (total - MIDS) * quarter - held)
            def _():
                send_to(m % 2, m // 2, 1, [far_mid[i % quarter]])

    wait_hands(r_recv, 0, 1)
    mirror = r_all.at[r_rows, pl.ds(pl.multiple_of(mirror_x * rows, rows), rows)]
    for device in near:
        hand(mirror, mirror, 2, device)
    wait_hands(r_send, 0, 1)
    for i in (1, 2):
        wait_hands(r_recv, i, len(near))
        wait_hands(r_send, i, len(near))
    @pl.when(is_end)
    def _():
        pl.semaphore_wait(crossed, len(other))
        tell(all_known, group, near_mid)

    @pl.when(~is_end)
    def _():
        pl.semaphore_wait(all_known, 1)

    for g in other:
        pltpu.make_async_remote_copy(
            src_ref=r_all.at[r_rows, :], dst_ref=r_all.at[r_rows, :], send_sem=f_send, recv_sem=f_recv,
            device_id=(g, me), device_id_type=MESH_IDS,
        ).start()
    many = r_all.at[pl.ds(0, (groups - 1) * r_cols), :]
    pltpu.make_async_copy(many, many, f_recv).wait()
    pltpu.make_async_copy(many, many, f_send).wait()
    for c in range(orr.shape[0] // 128):
        span = slice(c * 128, (c + 1) * 128)
        orr[span, :] = r_all[:, span].astype(jnp.float32).T.astype(jnp.bfloat16)

    def drain(p, carry):
        for a in range(2):
            by_left_out(a, p, functools.partial(wait_sends, a, p))
        return carry

    lax.fori_loop(max(pairs - SLOTS // 2, 0), pairs, drain, 0)

    def wait_recv(a, p, blocks):
        many = outs[a].at[pl.ds(2 * p, 2), :, pl.ds(0, blocks * rows)]
        pltpu.make_async_copy(many, many, recv.at[a, p]).wait()

    def arrive(p, carry):
        for a in range(2):
            by_left_out(a, p, functools.partial(wait_recv, a, p))
        return carry

    lax.fori_loop(0, pairs, arrive, 0)


def second_kernel(n, stash, after, land, send, recv):
    group, me = lax.axis_index("expert"), lax.axis_index("shard")
    is_end, far_end, far_mid, _ = peers(me, n)
    quarter = n // 4
    part, rows = stash.shape[1] // quarter, stash.shape[2]
    x = me % quarter
    barrier = pltpu.get_barrier_semaphore()
    for i in range(quarter):
        device = jnp.where(is_end, far_end[i], far_mid[i])
        pl.semaphore_signal(barrier, inc=1, device_id=(group, device), device_id_type=MESH_IDS)
    pl.semaphore_wait(barrier, quarter)

    def exchange(first, base, start):
        for i in range(quarter):
            to = (start + i) % quarter
            for m in range(first, ENDS):
                pltpu.make_async_remote_copy(
                    src_ref=stash.at[m, pl.ds(pl.multiple_of(to * part, part), part), :],
                    dst_ref=land.at[m, :, pl.ds(pl.multiple_of(x * rows, rows), rows)],
                    send_sem=send, recv_sem=recv, device_id=(group, base + to), device_id_type=MESH_IDS,
                ).start()
        got, sent = land.at[pl.ds(first, ENDS - first)], stash.at[pl.ds(first, ENDS - first)]
        pltpu.make_async_copy(got, got, recv).wait()
        pltpu.make_async_copy(sent, sent, send).wait()

    @pl.when(is_end)
    def _():
        exchange(0, far_end[0], 0)

    @pl.when(~is_end)
    def _():
        exchange(ENDS - MIDS, far_mid[0], x + 1)


def second(n, stash, after):
    _, span, rows = stash.shape
    quarter = n // 4
    anywhere = pl.BlockSpec(memory_space=pl.ANY)
    return pl.pallas_call(
        functools.partial(second_kernel, n),
        out_shape=pltpu.VMEM((ENDS, span // quarter, quarter * rows), stash.dtype),
        in_specs=[anywhere, anywhere],
        out_specs=anywhere,
        scratch_shapes=[pltpu.SemaphoreType.DMA, pltpu.SemaphoreType.DMA],
        compiler_params=pltpu.CompilerParams(
            collective_id=1, has_side_effects=True, vmem_limit_bytes=1024 * 1024,
        ),
        name="second",
    )(stash, after)


def fill_kernel(n, gate, up, land, og, ou, done):
    me = lax.axis_index("shard")
    is_end, far_end, far_mid, _ = peers(me, n)
    experts, width = gate.shape[0], land.shape[2]
    rows = width // (n // 4)

    def place(first, base):
        spot = pl.ds(pl.multiple_of(base * rows, width), width)
        copies = []
        for i in range(first, ENDS):
            m = 2 * experts - ENDS + i
            copies.append(pltpu.make_async_copy(land.at[i], (og, ou)[m % 2].at[m // 2, :, spot], done.at[i]))
        for copy in copies:
            copy.start()
        for copy in copies:
            copy.wait()

    @pl.when(is_end)
    def _():
        place(0, far_end[0])

    @pl.when(~is_end)
    def _():
        place(ENDS - MIDS, far_mid[0])


def fill(n, gate, up, land):
    anywhere = pl.BlockSpec(memory_space=pl.ANY)
    return pl.pallas_call(
        functools.partial(fill_kernel, n),
        out_shape=tuple(pltpu.HBM(x.shape, x.dtype) for x in (gate, up)),
        in_specs=[anywhere] * 3,
        out_specs=(anywhere,) * 2,
        scratch_shapes=[pltpu.SemaphoreType.DMA((ENDS,))],
        input_output_aliases={0: 0, 1: 1},
        compiler_params=pltpu.CompilerParams(vmem_limit_bytes=1024 * 1024),
        name="fill",
    )(gate, up, land)


PIECES = 4


def put_kernel(gate, up, router, og, ou, orr, after, done, done_router):
    size = gate.shape[0] // PIECES
    copies = [
        pltpu.make_async_copy(src.at[pl.ds(i * size, size)], dst.at[pl.ds(i * size, size)], done.at[a, i])
        for i in range(PIECES)
        for a, (src, dst) in enumerate(((gate, og), (up, ou)))
    ]
    copies.append(pltpu.make_async_copy(router, orr, done_router))
    for copy in copies:
        copy.start()
    for copy in copies:
        copy.wait()


def put(*held):
    anywhere = pl.BlockSpec(memory_space=pl.ANY)
    return pl.pallas_call(
        put_kernel,
        out_shape=tuple(pltpu.HBM(x.shape, x.dtype) for x in held) + (pltpu.VMEM((8, 128), jnp.float32),),
        in_specs=[anywhere] * len(held),
        out_specs=(anywhere,) * (len(held) + 1),
        scratch_shapes=[pltpu.SemaphoreType.DMA((2, PIECES)), pltpu.SemaphoreType.DMA],
        compiler_params=pltpu.CompilerParams(vmem_limit_bytes=1024 * 1024),
        name="put",
    )(*held)


def fused(n, groups, master_gate, second_gate, master_up, second_up, router_weight, router_gain):
    experts, rows, inner = master_gate.shape
    r_cols = router_weight.shape[1]
    final = (experts, inner // n, rows * n)
    anywhere = pl.BlockSpec(memory_space=pl.ANY)
    dma, regular = pltpu.SemaphoreType.DMA, pltpu.SemaphoreType.REGULAR
    *held, stash = pl.pallas_call(
        functools.partial(regroup_kernel, n, groups),
        out_shape=(
            pltpu.VMEM(final, jnp.bfloat16),
            pltpu.VMEM(final, jnp.bfloat16),
            jax.ShapeDtypeStruct((rows * n, r_cols * groups), jnp.bfloat16),
            pltpu.VMEM((ENDS, inner // 4, rows), jnp.bfloat16),
        ),
        in_specs=[anywhere] * 6,
        out_specs=(anywhere, anywhere, pl.BlockSpec(memory_space=pltpu.VMEM), pl.BlockSpec(memory_space=pltpu.VMEM)),
        scratch_shapes=[
            pltpu.VMEM((2, LOADS, rows, inner), jnp.float32),
            pltpu.VMEM((2, LOADS, rows, inner), jnp.bfloat16),
            pltpu.VMEM((2, SLOTS, inner, rows), jnp.bfloat16),
            pltpu.VMEM((r_cols, rows), jnp.float32),
            pltpu.VMEM((1, rows), jnp.float32),
            pltpu.VMEM((r_cols, rows), jnp.bfloat16),
            pltpu.VMEM((r_cols * groups, rows * n), jnp.bfloat16),
            dma((2, LOADS)), dma((2, LOADS)), dma((2,)),
            dma((2, SLOTS // 2)), dma((2, SLOTS // 2)), dma((2, experts // 2)),
            dma((3,)), dma((3,)), dma, dma,
            regular, regular, regular,
        ],
        compiler_params=pltpu.CompilerParams(
            collective_id=0, has_side_effects=True, vmem_limit_bytes=24 * 1024 * 1024,
        ),
        name="regroup",
    )(
        master_gate, second_gate, master_up, second_up,
        pltpu.with_memory_space_constraint(router_weight.T, pltpu.HBM),
        pltpu.with_memory_space_constraint(router_gain[None, :], pltpu.HBM),
    )
    gate, up, router, after = put(*held)
    return *fill(n, gate, up, second(n, stash, after)), router


def solution(mesh):
    n, groups = mesh.shape["shard"], mesh.shape["expert"]

    def shards(*args):
        experts, rows, inner = args[0].shape
        r_cols = args[4].shape[1]
        fits = (
            n % 8 == 0 and groups > 1 and rows % 128 == 0 and inner % 128 == 0
            and (inner // n) % 16 == 0 and r_cols % 16 == 0 and experts % PIECES == 0 and experts % 2 == 0 and experts // 2 > max(SLOTS // 2, EARLY // 4) + late_pairs(n) and ENDS >= MIDS
            and late_pairs(n) <= SLOTS // 2
        )
        return fused(n, groups, *args) if fits else plain(*args)

    in_specs = (
        P("expert", "shard", None),
        P("expert", "shard", None),
        P("expert", "shard", None),
        P("expert", "shard", None),
        P("shard", "expert"),
        P("shard"),
    )
    out_specs = (P("expert", "shard", None), P("expert", "shard", None), P())
    return jax.shard_map(shards, mesh=mesh, in_specs=in_specs, out_specs=out_specs, check_vma=False)
```
